16 devices in a mesh: data: 4 (over z, y), stage: 4 (over x, core).
Axes of the slice: x: 2, y: 2, z: 2, core: 2. Of those that a mesh axis runs over, the one named last changes fastest.
Arguments:
- X: bfloat16 [16, 512, 1536], P('data'), parts along dimension 0
- G: bfloat16 [16, 512, 1536], P('data'), parts along dimension 0
- W1: bfloat16 [4, 1536, 6144], P('stage')
- W2: bfloat16 [4, 6144, 1536], P('stage')
Outputs:
- output 1: bfloat16 [16, 512, 1536], P('data'), parts along dimension 0
- output 2: bfloat16 [16, 512, 1536], P('data'), parts along dimension 0
- output 3: float32 [16, 1536, 6144], P(('data', 'stage')), parts along dimension 0
- output 4: float32 [16, 6144, 1536], P(('data', 'stage')), parts along dimension 0
There are 4 independent parts. The reference program is written for one: setup_inputs(seed, part) draws one part's arguments, and reference() takes and returns one part's arrays. A program takes and returns all parts, laid end to end along the dimension named above; an argument that names none is the same for every part.
All inputs are finite; a program needn't handle non-finite values.
Results may differ from the reference program's by a relative error of at most 0.00963606.
Values are sent between devices in bfloat16 or wider.
A program may use at most 1 GiB of HBM per device.

```python
import jax
import jax.numpy as jnp
from jax import lax

D = 1536
F = 6144
LAYERS = 4
M = 4
B = 512


def setup_inputs(seed: int = 0, part: int = 0) -> dict:
    key = jax.random.PRNGKey(seed)
    ks, kpb = jax.random.split(key)
    kp = jax.random.fold_in(kpb, part)
    kx, kg = jax.random.split(kp)
    k1, k2 = jax.random.split(ks)
    X = jax.random.normal(kx, (M, B, D), jnp.float32).astype(jnp.bfloat16)
    G = jax.random.normal(kg, (M, B, D), jnp.float32).astype(jnp.bfloat16)
    W1 = (jax.random.normal(k1, (LAYERS, D, F), jnp.float32) * D ** -0.5).astype(jnp.bfloat16)
    W2 = (jax.random.normal(k2, (LAYERS, F, D), jnp.float32) * (F * LAYERS) ** -0.5).astype(jnp.bfloat16)
    return {'X': X, 'G': G, 'W1': W1, 'W2': W2}


def _fwd_layer(h, w1, w2):
    z = jnp.dot(h, w1, preferred_element_type=jnp.float32)
    u = jax.nn.gelu(z, approximate=True).astype(jnp.bfloat16)
    return (h.astype(jnp.float32) + jnp.dot(u, w2, preferred_element_type=jnp.float32)).astype(jnp.bfloat16)


def _bwd_layer(h, g, w1, w2):
    z = jnp.dot(h, w1, preferred_element_type=jnp.float32)
    u, gelu_vjp = jax.vjp(lambda t: jax.nn.gelu(t, approximate=True), z)
    du = jnp.dot(g, w2.T, preferred_element_type=jnp.float32)
    dz = gelu_vjp(du)[0].astype(jnp.bfloat16)
    dw2 = jnp.dot(u.astype(jnp.bfloat16).T, g, preferred_element_type=jnp.float32)
    dw1 = jnp.dot(h.T, dz, preferred_element_type=jnp.float32)
    dh = (g.astype(jnp.float32) + jnp.dot(dz, w1.T, preferred_element_type=jnp.float32)).astype(jnp.bfloat16)
    return dh, dw1, dw2


def reference(X, G, W1, W2):
    def one(carry, xg):
        a1, a2 = carry
        x, g = xg

        def fstep(h, w):
            return _fwd_layer(h, w[0], w[1]), h
        y, hs = lax.scan(fstep, x, (W1, W2))

        def bstep(gh, inp):
            w1, w2, h, c1, c2 = inp
            dh, dw1, dw2 = _bwd_layer(h, gh, w1, w2)
            return dh, (c1 + dw1, c2 + dw2)
        dx, (a1, a2) = lax.scan(bstep, g, (W1, W2, hs, a1, a2), reverse=True)
        return (a1, a2), (y, dx)

    init = (jnp.zeros(W1.shape, jnp.float32), jnp.zeros(W2.shape, jnp.float32))
    (dW1, dW2), (Y, dX) = lax.scan(one, init, (X, G))
    return Y, dX, dW1, dW2
```

```python
import functools

import jax
import jax.numpy as jnp
from jax import lax
from jax.experimental import pallas as pl
from jax.experimental.pallas import tpu as pltpu
from jax.sharding import PartitionSpec as P

MESH = pl.DeviceIdType.MESH
BF = jnp.bfloat16
F32 = jnp.float32
C0 = 0.7978845608028654
C1 = C0 * 0.044715


def _gelu(z):
    t = jnp.tanh(z * (C0 + C1 * (z * z)))
    h = 0.5 * z
    return h + h * t


def _dgelu(z):
    z2 = z * z
    t = jnp.tanh(z * (C0 + C1 * z2))
    return 0.5 * (1.0 + t) + (0.5 * z) * (1.0 - t * t) * (C0 + (3.0 * C1) * z2)


def _dot(a, b):
    return jnp.dot(a, b, preferred_element_type=F32)


def _dot_t(a, b):
    return lax.dot_general(a, b, (((1,), (1,)), ((), ())), preferred_element_type=F32)


def _pass_kernel(C, T, S, NT, x_hbm, g_hbm, w1_hbm, w2_hbm,
                 y, dx, hs, gs, us, dzs, zb,
                 w1, w2, h, g, ub, zs, obf, obb,
                 wsem, hsem, gsem, ysem, dxsem, fsem, bsem, ysend, dsend, hss, gss, zsem, usem):
    n_tok, D = h.shape
    F = w1.shape[1]
    nch, nt, nn = n_tok // C, F // T, D // NT
    s = lax.axis_index("stage")
    first, last = s == 0, s == 3

    def rows(c):
        return pl.ds(pl.multiple_of(c * C, C), C)

    def cols(n):
        return pl.ds(n * NT, NT)

    def local(src, dst, sem):
        return pltpu.make_async_copy(src, dst, sem)

    def got(ref, c, n, sem):
        v = ref.at[rows(c), cols(n)]
        return local(v, v, sem.at[c, n])

    def remote(src, dst, ssem, rsem, to):
        return pltpu.make_async_remote_copy(src, dst, ssem, rsem, device_id={"stage": to}, device_id_type=MESH)

    cw1 = local(w1_hbm, w1, wsem.at[0])
    cw2 = local(w2_hbm, w2, wsem.at[1])

    @pl.when(first)
    def _():
        for n in range(nn):
            local(x_hbm.at[rows(0), cols(n)], h.at[rows(0), cols(n)], hsem.at[0, n]).start()
    cw1.start()
    cw2.start()

    @pl.when(first)
    def _():
        for c in range(1, nch):
            for n in range(nn):
                local(x_hbm.at[rows(c), cols(n)], h.at[rows(c), cols(n)], hsem.at[c, n]).start()

    @pl.when(last)
    def _():
        for c in range(nch):
            for n in range(nn):
                local(g_hbm.at[rows(c), cols(n)], g.at[rows(c), cols(n)], gsem.at[c, n]).start()

    barrier = pltpu.get_barrier_semaphore()
    for d in range(1, 4):
        pl.semaphore_signal(barrier, inc=1, device_id={"stage": lax.rem(s + d, 4)}, device_id_type=MESH)
    pl.semaphore_wait(barrier, 3)
    cw1.wait()
    cw2.wait()

    def f_next(c, n):
        return remote(obf.at[c % 2, :, cols(n)], h.at[rows(c), cols(n)], fsem.at[c % 2, n], hsem.at[c, n], s + 1)

    def b_next(c, n):
        return remote(obb.at[c % 2, :, cols(n)], g.at[rows(c), cols(n)], bsem.at[c % 2, n], gsem.at[c, n], s - 1)

    def y_copies(c, n):
        src, dst = obf.at[c % 2, :, cols(n)], y.at[rows(c), cols(n)]
        return [remote(src, dst, ysend.at[1, c % 2, n], ysem.at[c, n], 1),
                remote(src, dst, ysend.at[2, c % 2, n], ysem.at[c, n], 2),
                local(src, dst, ysend.at[0, c % 2, n])]

    def dx_copies(c, n):
        src, dst = obb.at[c % 2, :, cols(n)], dx.at[rows(c), cols(n)]
        return [remote(src, dst, dsend.at[1, c % 2, n], dxsem.at[c, n], 2),
                remote(src, dst, dsend.at[2, c % 2, n], dxsem.at[c, n], 1),
                local(src, dst, dsend.at[0, c % 2, n])]

    def wait_sent(copies):
        for cp in copies[:-1]:
            cp.wait_send()
        copies[-1].wait()

    def f_wait(c):
        for n in range(nn):
            @pl.when(last)
            def _(n=n):
                wait_sent(y_copies(c, n))

            @pl.when(jnp.logical_not(last))
            def _(n=n):
                f_next(c, n).wait_send()

    def b_wait(c):
        for n in range(nn):
            @pl.when(first)
            def _(n=n):
                wait_sent(dx_copies(c, n))

            @pl.when(jnp.logical_not(first))
            def _(n=n):
                b_next(c, n).wait_send()

    def y_fwd(c, n):
        v = y.at[rows(c), cols(n)]
        return remote(v, v, ysend.at[0, c % 2, n], ysem.at[c, n], 0)

    def dx_fwd(c, n):
        v = dx.at[rows(c), cols(n)]
        return remote(v, v, dsend.at[0, c % 2, n], dxsem.at[c, n], 3)

    def z_out(c, j, k):
        return local(zs.at[k], zb.at[c, j], zsem.at[k])

    def z_in(c, j, k):
        return local(zb.at[c, j], zs.at[k], zsem.at[k])

    def save(dst, c):
        return local(ub, dst.at[rows(c), :], usem)

    def keep(src, dst, c, sem):
        return local(src.at[rows(c), :], dst.at[rows(c), :], sem.at[c])

    def fwd(c):
        for n in range(nn):
            got(h, c, n, hsem).wait()
        keep(h, hs, c, hss).start()
        hc = h.at[rows(c), :]

        def st1(j, _):
            k = j % 2

            @pl.when(j >= 2)
            def _():
                z_out(c, j - 2, k).wait()
            for i in range(T // S):
                col = pl.ds(pl.multiple_of(j * T + i * S, S), S)
                z = _dot(hc[...], w1[:, col])
                zs[k, :, i * S:(i + 1) * S] = z
                ub[:, col] = _gelu(z).astype(BF)
            z_out(c, j, k).start()
            return 0
        lax.fori_loop(0, nt, st1, 0)
        save(us, c).start()

        @pl.when(c >= 2)
        def _():
            f_wait(c - 2)

        def st2(n, _):
            col = pl.ds(pl.multiple_of(n * NT, NT), NT)
            obf[c % 2, :, col] = (hc[:, col].astype(F32) + _dot(ub[...], w2[:, col])).astype(BF)

            @pl.when(last)
            def _():
                src, dst = obf.at[c % 2, :, col], y.at[rows(c), col]
                remote(src, dst, ysend.at[1, c % 2, n], ysem.at[c, n], 1).start()
                remote(src, dst, ysend.at[2, c % 2, n], ysem.at[c, n], 2).start()
                local(src, dst, ysend.at[0, c % 2, n]).start()

            @pl.when(jnp.logical_not(last))
            def _():
                remote(obf.at[c % 2, :, col], h.at[rows(c), col], fsem.at[c % 2, n], hsem.at[c, n], s + 1).start()
            return 0
        lax.fori_loop(0, nn, st2, 0)
        for j in range(max(0, nt - 2), nt):
            z_out(c, j, j % 2).wait()
        save(us, c).wait()

    def bwd(c):
        z_in(c, 0, 0).start()
        for n in range(nn):
            got(g, c, n, gsem).wait()
        keep(g, gs, c, gss).start()
        gc = g.at[rows(c), :]

        def st1(j, _):
            k = j % 2

            @pl.when(j + 1 < nt)
            def _():
                z_in(c, j + 1, 1 - k).start()
            z_in(c, j, k).wait()
            for i in range(T // S):
                col = pl.ds(pl.multiple_of(j * T + i * S, S), S)
                du = _dot_t(gc[...], w2[col, :])
                ub[:, col] = (_dgelu(zs[k, :, i * S:(i + 1) * S]) * du).astype(BF)
            return 0
        lax.fori_loop(0, nt, st1, 0)
        save(dzs, c).start()

        @pl.when(c >= 2)
        def _():
            b_wait(c - 2)

        def st2(n, _):
            col = pl.ds(pl.multiple_of(n * NT, NT), NT)
            obb[c % 2, :, col] = (gc[:, col].astype(F32) + _dot_t(ub[...], w1[col, :])).astype(BF)

            @pl.when(first)
            def _():
                src, dst = obb.at[c % 2, :, col], dx.at[rows(c), col]
                remote(src, dst, dsend.at[1, c % 2, n], dxsem.at[c, n], 2).start()
                remote(src, dst, dsend.at[2, c % 2, n], dxsem.at[c, n], 1).start()
                local(src, dst, dsend.at[0, c % 2, n]).start()

            @pl.when(jnp.logical_not(first))
            def _():
                remote(obb.at[c % 2, :, col], g.at[rows(c), col], bsem.at[c % 2, n], gsem.at[c, n], s - 1).start()
            return 0
        lax.fori_loop(0, nn, st2, 0)
        save(dzs, c).wait()

        @pl.when(s == 1)
        def _():
            @pl.when(c >= 2)
            def _():
                for n in range(nn):
                    y_fwd(c - 2, n).wait_send()
            for n in range(nn):
                got(y, c, n, ysem).wait()
                y_fwd(c, n).start()

        @pl.when((s == 2) & (c >= 3))
        def _():
            pass_dx(c - 3)

    def pass_dx(c):
        @pl.when(c >= 2)
        def _():
            for n in range(nn):
                dx_fwd(c - 2, n).wait_send()
        for n in range(nn):
            got(dx, c, n, dxsem).wait()
            dx_fwd(c, n).start()

    def step(t, _):
        is_f = jnp.where(last, t % 2 == 0, t < nch)
        c = jnp.where(last, t // 2, jnp.where(t < nch, t, t - nch))

        @pl.when(is_f)
        def _():
            fwd(c)

        @pl.when(jnp.logical_not(is_f))
        def _():
            bwd(c)
        return 0
    lax.fori_loop(0, 2 * nch, step, 0)

    @pl.when(s == 2)
    def _():
        def rest(c, _):
            pass_dx(c)
            return 0
        lax.fori_loop(nch - 3, nch, rest, 0)

    def drain(c, _):
        f_wait(c)
        b_wait(c)

        @pl.when(s == 1)
        def _():
            for n in range(nn):
                y_fwd(c, n).wait_send()

        @pl.when(s == 2)
        def _():
            for n in range(nn):
                dx_fwd(c, n).wait_send()
        return 0
    lax.fori_loop(nch - 2, nch, drain, 0)

    def arrivals(c, _):
        keep(h, hs, c, hss).wait()
        keep(g, gs, c, gss).wait()
        for n in range(nn):
            @pl.when((s == 0) | (s == 2))
            def _(n=n):
                got(y, c, n, ysem).wait()

            @pl.when((s == 1) | (s == 3))
            def _(n=n):
                got(dx, c, n, dxsem).wait()
        return 0
    lax.fori_loop(0, nch, arrivals, 0)


def _run_pass(x, g, w1, w2, C=256, T=1536, S=512, NT=512):
    n_tok, D = x.shape
    F = w1.shape[1]
    nch, nt, nn = n_tok // C, F // T, D // NT
    any_ = pl.BlockSpec(memory_space=pl.ANY)
    act = jax.ShapeDtypeStruct((n_tok, D), BF)
    hid = jax.ShapeDtypeStruct((n_tok, F), BF)
    dma = pltpu.SemaphoreType.DMA
    return pl.pallas_call(
        functools.partial(_pass_kernel, C, T, S, NT),
        out_shape=(act, act, act, act, hid, hid, jax.ShapeDtypeStruct((nch, nt, C, T), F32)),
        in_specs=[any_] * 4,
        out_specs=(any_,) * 7,
        scratch_shapes=[
            pltpu.VMEM((D, F), BF), pltpu.VMEM((F, D), BF),
            pltpu.VMEM((n_tok, D), BF), pltpu.VMEM((n_tok, D), BF),
            pltpu.VMEM((C, F), BF), pltpu.VMEM((2, C, T), F32),
            pltpu.VMEM((2, C, D), BF), pltpu.VMEM((2, C, D), BF),
            dma((2,)), dma((nch, nn)), dma((nch, nn)), dma((nch, nn)), dma((nch, nn)),
            dma((2, nn)), dma((2, nn)), dma((3, 2, nn)), dma((3, 2, nn)),
            dma((nch,)), dma((nch,)), dma((2,)), dma,
        ],
        compiler_params=pltpu.CompilerParams(collective_id=0, has_side_effects=True, vmem_limit_bytes=67043328),
        name="mlp_pass",
    )(x, g, w1, w2)


def _dot_k0(a, b):
    return lax.dot_general(a, b, (((0,), (0,)), ((), ())), preferred_element_type=F32)


def solution(mesh):
    def body(x, g, w1, w2):
        shape = x.shape
        D = shape[-1]
        y, dx, hs, gs, us, dzs, _ = _run_pass(x.reshape(-1, D), g.reshape(-1, D), w1[0], w2[0])
        dw1 = _dot_k0(hs, dzs)
        dw2 = _dot_k0(us, gs)
        return y.reshape(shape), dx.reshape(shape), dw1[None], dw2[None]

    return jax.shard_map(body, mesh=mesh,
                         in_specs=(P('data'), P('data'), P('stage'), P('stage')),
                         out_specs=(P('data'), P('data'), P(('data', 'stage')), P(('data', 'stage'))),
                         check_vma=False)
```

```python
import functools

import jax
import jax.numpy as jnp
from jax import lax
from jax.experimental import pallas as pl
from jax.experimental.pallas import tpu as pltpu
from jax.sharding import PartitionSpec as P

MESH = pl.DeviceIdType.MESH
BF = jnp.bfloat16
F32 = jnp.float32
C0 = 0.7978845608028654
C1 = C0 * 0.044715


def _act(z):
    q = C1 * (z * z)
    p = q + C0
    s = 1.0 + jnp.tanh(z * p)
    h = 0.5 * z
    return h * s, s * (0.5 + h * (2.0 - s) * (p + 2.0 * q))


def _dot(a, b):
    return jnp.dot(a, b, preferred_element_type=F32)


def _dot_t(a, b):
    return lax.dot_general(a, b, (((1,), (1,)), ((), ())), preferred_element_type=F32)


def _pass_kernel(C, T, NT, x_hbm, g_hbm, w1_hbm, w2_hbm,
                 y, dx, hs, gs, us, dzs, gb,
                 w1, w2, hg, ub, za, zb, gp, obf, obb,
                 wsem, hsem, gsem, ysem, dxsem, fsem, bsem, ysend, dsend, hss, gss, gsem2, usem):
    n_tok, D = x_hbm.shape
    F = w1.shape[1]
    hf = n_tok // C // 2
    nch, npair, nn = n_tok // C, F // (2 * T), D // NT
    s = lax.axis_index("stage")
    first, last = s == 0, s == 3
    inner = jnp.logical_not(last)

    def rows(c):
        return pl.ds(pl.multiple_of(c * C, C), C)

    def grows(c):
        return rows(jnp.where(c < hf, nch + c, c - hf))

    def cols(n):
        return pl.ds(n * NT if isinstance(n, int) else pl.multiple_of(n * NT, NT), NT)

    def local(src, dst, sem):
        return pltpu.make_async_copy(src, dst, sem)

    def got(ref, r, c, n, sem):
        v = ref.at[r, cols(n)]
        return local(v, v, sem.at[c, n])

    def remote(src, dst, ssem, rsem, to):
        return pltpu.make_async_remote_copy(src, dst, ssem, rsem, device_id={"stage": to}, device_id_type=MESH)

    def g_load(c, n):
        return local(g_hbm.at[rows(c), cols(n)], hg.at[grows(c), cols(n)], gsem.at[c, n])

    def w1_load(j):
        col = pl.ds(pl.multiple_of(j * T, T), T)
        return local(w1_hbm.at[:, col], w1.at[:, col], wsem.at[j])

    w2_load = local(w2_hbm, w2, wsem.at[F // T])

    @pl.when(first)
    def _():
        for n in range(nn):
            local(x_hbm.at[rows(0), cols(n)], hg.at[rows(0), cols(n)], hsem.at[0, n]).start()
    for j in range(F // T):
        w1_load(j).start()
    w2_load.start()

    @pl.when(first)
    def _():
        for c in range(1, nch):
            for n in range(nn):
                local(x_hbm.at[rows(c), cols(n)], hg.at[rows(c), cols(n)], hsem.at[c, n]).start()

    @pl.when(last)
    def _():
        for c in range(hf):
            for n in range(nn):
                g_load(c, n).start()

    barrier = pltpu.get_barrier_semaphore()
    for d in range(1, 4):
        pl.semaphore_signal(barrier, inc=1, device_id={"stage": lax.rem(s + d, 4)}, device_id_type=MESH)
    pl.semaphore_wait(barrier, 3)

    def f_next(c, n):
        return remote(obf.at[:, cols(n)], hg.at[rows(c), cols(n)], fsem.at[c % 2, n], hsem.at[c, n], s + 1)

    def b_next(c, n):
        return remote(obb.at[:, cols(n)], hg.at[grows(c), cols(n)], bsem.at[c % 2, n], gsem.at[c, n], s - 1)

    def y_copies(c, n):
        src, dst = obf.at[:, cols(n)], y.at[rows(c), cols(n)]
        return [remote(src, dst, ysend.at[1, c % 2, n], ysem.at[c, n], 1),
                remote(src, dst, ysend.at[2, c % 2, n], ysem.at[c, n], 2),
                local(src, dst, ysend.at[0, c % 2, n])]

    def dx_copies(c, n):
        src, dst = obb.at[:, cols(n)], dx.at[rows(c), cols(n)]
        return [remote(src, dst, dsend.at[1, c % 2, n], dxsem.at[c, n], 2),
                remote(src, dst, dsend.at[2, c % 2, n], dxsem.at[c, n], 1),
                local(src, dst, dsend.at[0, c % 2, n])]

    def wait_sent(copies):
        for cp in copies[:-1]:
            cp.wait_send()
        copies[-1].wait()

    def f_wait(c):
        for n in range(nn):
            @pl.when(last)
            def _(n=n):
                wait_sent(y_copies(c, n))

            @pl.when(jnp.logical_not(last))
            def _(n=n):
                f_next(c, n).wait_send()

    def b_wait(c):
        for n in range(nn):
            @pl.when(first)
            def _(n=n):
                wait_sent(dx_copies(c, n))

            @pl.when(jnp.logical_not(first))
            def _(n=n):
                b_next(c, n).wait_send()

    def y_fwd(c, n):
        v = y.at[rows(c), cols(n)]
        return remote(v, v, ysend.at[0, c % 2, n], ysem.at[c, n], 0)

    def dx_fwd(c, n):
        v = dx.at[rows(c), cols(n)]
        return remote(v, v, dsend.at[0, c % 2, n], dxsem.at[c, n], 3)

    def gp_out(c, i):
        return local(gp.at[i], gb.at[c, i], gsem2.at[i])

    def gp_in(c, i):
        return local(gb.at[c, i], gp.at[i], gsem2.at[i])

    def save(dst, c):
        return local(ub, dst.at[rows(c), :], usem.at[0])

    def u_head(c):
        return local(ub.at[:, :F - 2 * T], us.at[rows(c), :F - 2 * T], usem.at[1])

    def u_tail(c):
        return local(ub.at[:, F - 2 * T:], us.at[rows(c), F - 2 * T:], usem.at[2])

    def keep(r, dst, c, sem):
        return local(hg.at[r, :], dst.at[rows(c), :], sem.at[c])

    def fwd(c):
        for n in range(nn):
            got(hg, rows(c), c, n, hsem).wait()
        keep(rows(c), hs, c, hss).start()
        hc = hg.at[rows(c), :]

        def act(zr, k, half, off):
            for r in range(0, C, 16):
                u, d = _act(zr[r:r + 16])
                ub[r:r + 16, pl.ds(off, T)] = u.astype(BF)
                gp[k, half, r:r + 16] = d

        def zdot(zr, off):
            for j in range(0, T, NT):
                zr[:, j:j + NT] = _dot(hc[...], w1[:, pl.ds(off + j, NT)])

        @pl.when(c == 0)
        def _():
            w1_load(0).wait()
        zdot(za, 0)

        def st1(i, _):
            @pl.when(inner & (c >= 1))
            def _():
                gp_out(c - 1, i).wait()

            @pl.when(c == 0)
            def _():
                w1_load(2 * i + 1).wait()
                w1_load(2 * i + 2).wait()
            o = pl.multiple_of(2 * i * T, 2 * T)
            act(za, i, 0, o)
            zdot(zb, o + T)
            act(zb, i, 1, o + T)
            zdot(za, o + 2 * T)

            @pl.when(inner)
            def _():
                gp_out(c, i).start()
            return 0
        lax.fori_loop(0, npair - 1, st1, 0)
        u_head(c).start()
        i = npair - 1
        o = 2 * i * T

        @pl.when(c >= 1)
        def _():
            f_wait(c - 1)

        @pl.when(inner & (c >= 1))
        def _():
            gp_out(c - 1, i).wait()
            u_tail(c - 1).wait()

        @pl.when(c == 0)
        def _():
            w1_load(F // T - 1).wait()
            w2_load.wait()
        act(za, i, 0, o)
        zdot(zb, o + T)
        def out(n, col, a):
            obf[:, col] = (hc[:, col].astype(F32) + a).astype(BF)

            @pl.when(last)
            def _():
                for cp in y_copies(c, n):
                    cp.start()

            @pl.when(inner)
            def _():
                f_next(c, n).start()

        keep(rows(c), hs, c, hss).wait()
        a = _dot(ub[:, :F - T], w2[:F - T, cols(0)])
        act(zb, i, 1, o + T)
        out(0, cols(0), a + _dot(ub[:, F - T:], w2[F - T:, cols(0)]))
        u_tail(c).start()

        def st2(n, _):
            out(n, cols(n), _dot(ub[...], w2[:, cols(n)]))
            return 0
        lax.fori_loop(1, nn, st2, 0)

        @pl.when(last & (c < hf))
        def _():
            for n in range(nn):
                g_load(c + hf, n).start()

        @pl.when(inner)
        def _():
            gp_out(c, i).start()
        u_head(c).wait()

    def bwd(c):
        @pl.when(inner & (c == 0))
        def _():
            for i in range(npair):
                gp_out(nch - 1, i).wait()
                gp_in(0, i).start()
        for n in range(nn):
            got(hg, grows(c), c, n, gsem).wait()
        keep(grows(c), gs, c, gss).start()
        gc = hg.at[grows(c), :]

        def st1(i, _):
            @pl.when(inner)
            def _():
                gp_in(c, i).wait()

            @pl.when((i == npair - 1) & (last | (c == 0)))
            def _():
                u_tail(jnp.where(last, c, nch - 1)).wait()
            for q in range(2):
                for j in range(0, T, NT):
                    col = pl.ds(pl.multiple_of((2 * i + q) * T + j, NT), NT)
                    ub[:, col] = (gp[i, q, :, j:j + NT] * _dot_t(gc[...], w2[col, :])).astype(BF)
            return 0
        lax.fori_loop(0, npair, st1, 0)
        save(dzs, c).start()

        @pl.when(inner & (c + 1 < nch))
        def _():
            for i in range(npair):
                gp_in(c + 1, i).start()

        @pl.when(c >= 1)
        def _():
            b_wait(c - 1)
        def st2(n, _):
            col = cols(n)
            obb[:, col] = (gc[:, col].astype(F32) + _dot_t(ub[...], w1[col, :])).astype(BF)

            @pl.when(first)
            def _():
                for cp in dx_copies(c, n):
                    cp.start()

            @pl.when(jnp.logical_not(first))
            def _():
                b_next(c, n).start()
            return 0
        lax.fori_loop(0, nn, st2, 0)
        save(dzs, c).wait()

        @pl.when(s == 1)
        def _():
            @pl.when(c >= 2)
            def _():
                for n in range(nn):
                    y_fwd(c - 2, n).wait_send()
            for n in range(nn):
                got(y, rows(c), c, n, ysem).wait()
                y_fwd(c, n).start()

        @pl.when((s == 2) & (c >= 3))
        def _():
            pass_dx(c - 3)

    def pass_dx(c):
        @pl.when(c >= 2)
        def _():
            for n in range(nn):
                dx_fwd(c - 2, n).wait_send()
        for n in range(nn):
            got(dx, rows(c), c, n, dxsem).wait()
            dx_fwd(c, n).start()

    def step(t, _):
        is_f = jnp.where(last, t % 2 == 0, t < nch)
        c = jnp.where(last, t // 2, jnp.where(t < nch, t, t - nch))

        @pl.when(is_f)
        def _():
            fwd(c)

        @pl.when(jnp.logical_not(is_f))
        def _():
            bwd(c)
        return 0
    lax.fori_loop(0, 2 * nch, step, 0)

    @pl.when(s == 2)
    def _():
        def rest(c, _):
            pass_dx(c)
            return 0
        lax.fori_loop(nch - 3, nch, rest, 0)

    f_wait(nch - 1)
    b_wait(nch - 1)

    def drain(c, _):

        @pl.when(s == 1)
        def _():
            for n in range(nn):
                y_fwd(c, n).wait_send()

        @pl.when(s == 2)
        def _():
            for n in range(nn):
                dx_fwd(c, n).wait_send()
        return 0
    lax.fori_loop(nch - 2, nch, drain, 0)

    def arrivals(c, _):
        keep(grows(c), gs, c, gss).wait()
        for n in range(nn):
            @pl.when((s == 0) | (s == 2))
            def _(n=n):
                got(y, rows(c), c, n, ysem).wait()

            @pl.when((s == 1) | (s == 3))
            def _(n=n):
                got(dx, rows(c), c, n, dxsem).wait()
        return 0
    lax.fori_loop(0, nch, arrivals, 0)


def _run_pass(x, g, w1, w2, C=256, T=1024, NT=512):
    n_tok, D = x.shape
    F = w1.shape[1]
    nch, npair, nn = n_tok // C, F // (2 * T), D // NT
    any_ = pl.BlockSpec(memory_space=pl.ANY)
    act = jax.ShapeDtypeStruct((n_tok, D), BF)
    hid = jax.ShapeDtypeStruct((n_tok, F), BF)
    dma = pltpu.SemaphoreType.DMA
    return pl.pallas_call(
        functools.partial(_pass_kernel, C, T, NT),
        out_shape=(act, act, act, act, hid, hid, jax.ShapeDtypeStruct((nch, npair, 2, C, T), F32)),
        in_specs=[any_] * 4,
        out_specs=(any_,) * 7,
        scratch_shapes=[
            pltpu.VMEM((D, F), BF), pltpu.VMEM((F, D), BF),
            pltpu.VMEM((n_tok + n_tok // 2, D), BF),
            pltpu.VMEM((C, F), BF), pltpu.VMEM((C, T), F32), pltpu.VMEM((C, T), F32),
            pltpu.VMEM((npair, 2, C, T), F32),
            pltpu.VMEM((C, D), BF), pltpu.VMEM((C, D), BF),
            dma((F // T + 1,)), dma((nch, nn)), dma((nch, nn)), dma((nch, nn)), dma((nch, nn)),
            dma((2, nn)), dma((2, nn)), dma((3, 2, nn)), dma((3, 2, nn)),
            dma((nch,)), dma((nch,)), dma((npair,)), dma((3,)),
        ],
        compiler_params=pltpu.CompilerParams(collective_id=0, has_side_effects=True, vmem_limit_bytes=67043328),
        name="mlp_pass",
    )(x, g, w1, w2)


def _dot_k0(a, b):
    return lax.dot_general(a, b, (((0,), (0,)), ((), ())), preferred_element_type=F32)


def _grad_kernel(n1, x_any, g_any, yi, dxi, dz, u, yo, dxo, dw1, dw2, h, g, sem):
    i = pl.program_id(0)
    ch = pltpu.make_async_copy(x_any, h, sem.at[0])
    cg = pltpu.make_async_copy(g_any, g, sem.at[1])

    @pl.when(i == 0)
    def _():
        ch.start()
        cg.start()
        ch.wait()
    yo[...] = yi[...]
    dxo[...] = dxi[...]

    @pl.when(i < n1)
    def _():
        dw1[...] = _dot_k0(h[...], dz[...])

    @pl.when(i == n1)
    def _():
        cg.wait()

    @pl.when(i >= n1)
    def _():
        dw2[...] = _dot_k0(u[...], g[...])


def _run_grads(hs, gs, us, dzs, y, dx, B=512):
    n_tok, D = hs.shape
    F = us.shape[1]
    n1 = F // B
    R = n_tok // 16
    any_ = pl.BlockSpec(memory_space=pl.ANY)
    act = pl.BlockSpec((R, D), lambda i: (jnp.minimum(i, 15), 0))
    one = lambda i: jnp.minimum(i, n1 - 1)
    two = lambda i: jnp.maximum(i - n1, 0)
    flops = 4 * n_tok * D * F
    return pl.pallas_call(
        functools.partial(_grad_kernel, n1),
        grid=(2 * n1,),
        in_specs=[any_, any_, act, act,
                  pl.BlockSpec((n_tok, B), lambda i: (0, one(i))), pl.BlockSpec((n_tok, B), lambda i: (0, two(i)))],
        out_specs=(act, act, pl.BlockSpec((D, B), lambda i: (0, one(i))), pl.BlockSpec((B, D), lambda i: (two(i), 0))),
        out_shape=(jax.ShapeDtypeStruct((n_tok, D), BF), jax.ShapeDtypeStruct((n_tok, D), BF),
                   jax.ShapeDtypeStruct((D, F), F32), jax.ShapeDtypeStruct((F, D), F32)),
        scratch_shapes=[pltpu.VMEM((n_tok, D), BF), pltpu.VMEM((n_tok, D), BF), pltpu.SemaphoreType.DMA((2,))],
        compiler_params=pltpu.CompilerParams(dimension_semantics=("arbitrary",), vmem_limit_bytes=67043328),
        cost_estimate=pl.CostEstimate(flops=flops, bytes_accessed=200 * 1024 * 1024, transcendentals=0),
        name="mlp_grads",
    )(hs, gs, y, dx, dzs, us)


def solution(mesh):
    def body(x, g, w1, w2):
        shape = x.shape
        D = shape[-1]
        y, dx, hs, gs, us, dzs, _ = _run_pass(x.reshape(-1, D), g.reshape(-1, D), w1[0], w2[0])
        y, dx, dw1, dw2 = _run_grads(hs, gs, us, dzs, y, dx)
        return y.reshape(shape), dx.reshape(shape), dw1[None], dw2[None]

    return jax.shard_map(body, mesh=mesh,
                         in_specs=(P('data'), P('data'), P('stage'), P('stage')),
                         out_specs=(P('data'), P('data'), P(('data', 'stage')), P(('data', 'stage'))),
                         check_vma=False)
```
